32 devices in a mesh: section: 2 (over y), dp: 4 (over x, core), mp: 4 (over z).
Axes of the slice: x: 2, y: 2, z: 4, core: 2. Of those that a mesh axis runs over, the one named last changes fastest.
Arguments:
- patches: bfloat16 [4096, 1280], P(('section', 'dp')), may hold values from -6 to 6
- patch_counts: int32 [16], P(('section', 'dp')), may hold values from 64 to 256, as said below
- dest_rows: int32 [1024], P(('section', 'dp')), may hold values from 0 to 4095, as said below
- qkv_weight: bfloat16 [1280, 3, 1280], P(None, None, 'mp'), may hold values from -1 to 1
- out_weight: bfloat16 [1280, 1280], P('mp'), may hold values from -0.15625 to 0.15625
- attn_gain: bfloat16 [1280], replicated, may hold values from 0.25 to 1.75
- merge_gain: bfloat16 [1280], replicated, may hold values from 0.25 to 1.75
- fc1_weight: bfloat16 [5120, 5120], P('mp', ('section', 'dp')), may hold values from -0.078125 to 0.078125
- fc1_bias: bfloat16 [5120], P(('section', 'dp')), may hold values from -3 to 3
- fc2_weight: bfloat16 [5120, 8192], P(('section', 'dp'), 'mp'), may hold values from -0.078125 to 0.078125
- fc2_bias: bfloat16 [8192], P('mp'), may hold values from -3 to 3
- text_embeds: bfloat16 [4096, 8192], P(('section', 'dp'), 'mp'), may hold values from -6 to 6
- section_hidden: bfloat16 [4096, 8192], P(('section', 'dp'), 'mp'), may hold values from -80 to 80
- llm_gain: bfloat16 [8192], P('mp'), may hold values from 0.25 to 1.75
Outputs:
- sequence_embeds: bfloat16 [4096, 8192], P(('section', 'dp'), 'mp')
- layer_inputs: bfloat16 [4096, 8192], P(('section', 'dp'), 'mp')
The draws below stay inside these ranges and needn't reach their ends.
Inputs may be any that keep to these rules, and one draw needn't show every extreme that they name: `patch_counts`: multiples of 4; a tile's patches fill the first slots of its block. `dest_rows`: all rows differ. Each group's merged slots form runs of 16 consecutive slots (aligned); a run goes to one sequence slice (row // 512, numbered in section-major order), different runs of a group to different slices. Rows of slots that are not live are never written.
All inputs are finite; a program needn't handle non-finite values.
Results may differ from the reference program's by a relative error of at most 0.0055.
Values may be sent and summed in bfloat16 or wider, within the bound.
No kernel may reach another device: no remote copies, remote signals or barrier semaphores. Data moves between devices by JAX's collectives and lax.ppermute only.
A program may use at most 128 MiB of HBM per device.

```python
import math
import jax
import jax.numpy as jnp
from jax import lax

D_VIT = 1280
HEADS = 16
HEAD_DIM = 80
MERGE_HID = 5120
HID = 8192
BLOCK = 256
TILES_DEV = 2
SEQ_ROWS = 512
GROUPS = 8
P_DEV = 512
M_DEV = 128
CAP = 16
PATCHES = 4096
TILES = 16
MERGE_IN = 5120
RECV_ROWS = 4096
N_SECTION = 2
N_DP = 4


def draw_patch_counts(key, part):
    return (4 * jax.random.randint(key, (TILES,), CAP, BLOCK // 4 + 1)).astype(jnp.int32)


def draw_dest_rows(key, part):
    group_total = GROUPS
    run_total = M_DEV // CAP
    heavy = jax.random.randint(jax.random.fold_in(key, 1), (), 0, group_total).astype(jnp.int32)

    def run_order(order_key):
        others = (heavy + 1 + jax.random.permutation(order_key, group_total - 1).astype(jnp.int32)) % group_total
        return jnp.concatenate([heavy[None], others])[:run_total]
    targets = jax.vmap(run_order)(jax.random.split(jax.random.fold_in(key, 2), group_total))
    places = jax.vmap(lambda place_key: jax.random.permutation(place_key, SEQ_ROWS).astype(jnp.int32))(jax.random.split(jax.random.fold_in(key, 3), group_total))
    source = jnp.arange(group_total, dtype=jnp.int32)[:, None, None]
    lane = jnp.arange(CAP, dtype=jnp.int32)[None, None, :]
    receiver = jnp.broadcast_to(targets[:, :, None], (group_total, run_total, CAP))
    position = places[receiver, source * CAP + lane]
    return (receiver * SEQ_ROWS + position).reshape(-1).astype(jnp.int32)


def draw_qkv_weight(key, part):
    base = jax.random.normal(key, (D_VIT, 3, D_VIT), jnp.float32) * D_VIT ** (-0.5)
    base = jnp.clip(base, -0.15, 0.15)
    return base.astype(jnp.bfloat16)


def draw_section_hidden(key, part):
    noise = jax.random.normal(jax.random.fold_in(key, 1), (RECV_ROWS, HID), jnp.float32)
    column_scale = jnp.exp(jnp.linspace(0.0, math.log(10.0), HID))[None, :]
    row_scale = jnp.exp(jax.random.uniform(jax.random.fold_in(key, 2), (RECV_ROWS, 1), jnp.float32, 0.0, math.log(10.0)))
    return jnp.clip(0.1 * noise * column_scale * row_scale, -80.0, 80.0).astype(jnp.bfloat16)


def shard_levels(key, shape, pieces, low, high):
    loudness = 1.0
    for axis_at, blocks in pieces:
        draws = jax.random.uniform(jax.random.fold_in(jax.random.fold_in(key, 6), axis_at), (blocks,), jnp.float32, low / len(pieces), high / len(pieces))
        loudness = loudness * jnp.repeat(jnp.exp(draws), shape[axis_at] // blocks).reshape((-1,) + (1,) * (len(shape) - 1 - axis_at))
    return loudness


def gaussian(own_key, dims, scale, bound, shards=(), kind=jnp.bfloat16):
    array = scale * jax.random.normal(own_key, dims, jnp.float32)
    if shards:
        array = array * shard_levels(own_key, dims, shards, -0.22, 0.18)
    return jnp.clip(array, -bound, bound).astype(kind)


def setup_inputs(seed: int = 0) -> dict:
    streams_of = jax.random.split(jax.random.key(seed), 15)
    return {
        "patches": gaussian(streams_of[0], (PATCHES, D_VIT), 1.0, 6.0, ((0, 8),)),
        "patch_counts": draw_patch_counts(jax.random.fold_in(streams_of[14], 71), 0),
        "dest_rows": draw_dest_rows(jax.random.fold_in(streams_of[14], 71), 0),
        "qkv_weight": draw_qkv_weight(jax.random.fold_in(streams_of[14], 71), 0),
        "out_weight": gaussian(streams_of[4], (D_VIT, D_VIT), D_VIT ** -0.5, 0.15625, ((0, 4),)),
        "attn_gain": jnp.clip(1.0 + 0.15 * jax.random.normal(streams_of[5], (D_VIT,), jnp.float32), 0.25, 1.75).astype(jnp.bfloat16),
        "merge_gain": jnp.clip(1.0 + 0.15 * jax.random.normal(streams_of[6], (D_VIT,), jnp.float32), 0.25, 1.75).astype(jnp.bfloat16),
        "fc1_weight": gaussian(streams_of[7], (MERGE_IN, MERGE_HID), MERGE_IN ** -0.5, 0.078125, ((0, 4), (1, 8))),
        "fc1_bias": gaussian(streams_of[8], (MERGE_HID,), 0.5, 3.0, ((0, 8),)),
        "fc2_weight": gaussian(streams_of[9], (MERGE_HID, HID), MERGE_HID ** -0.5, 0.078125, ((0, 8), (1, 4))),
        "fc2_bias": gaussian(streams_of[10], (HID,), 0.5, 3.0, ((0, 4),)),
        "text_embeds": gaussian(streams_of[11], (RECV_ROWS, HID), 1.0, 6.0, ((0, 8), (1, 4))),
        "section_hidden": draw_section_hidden(jax.random.fold_in(streams_of[14], 71), 0),
        "llm_gain": jnp.clip(1.0 + 0.15 * jax.random.normal(streams_of[13], (HID,), jnp.float32), 0.25, 1.75).astype(jnp.bfloat16),
    }


vit_eps = 1e-06
llm_eps = 1e-06

def layer_norm(values, gain):
    centred = values.astype(jnp.float32)
    centred = centred - lax.optimization_barrier(jnp.mean(centred, axis=-1, keepdims=True))
    variance = lax.optimization_barrier(jnp.mean(centred * centred, axis=-1, keepdims=True))
    return centred * lax.rsqrt(variance + vit_eps) * gain.astype(jnp.float32)

def group_embed(group_rows, group_counts, qkv_weight, out_weight, attn_gain, merge_gain, fc1_weight, fc1_bias, fc2_weight, fc2_bias):
    normed_in = layer_norm(group_rows, attn_gain).astype(jnp.bfloat16)
    projections = jnp.dot(normed_in, qkv_weight.reshape(D_VIT, 3 * D_VIT), preferred_element_type=jnp.float32).astype(jnp.bfloat16)
    projections = projections.reshape(TILES_DEV, BLOCK, 3, HEADS, HEAD_DIM).astype(jnp.float32)
    query_part = projections[:, :, 0]
    key_part = projections[:, :, 1]
    value_part = projections[:, :, 2]
    scores = jnp.einsum('tqhd,tkhd->thqk', query_part, key_part) * HEAD_DIM ** (-0.5)
    key_live = jnp.arange(BLOCK, dtype=jnp.int32)[None, None, None, :] < group_counts[:, None, None, None]
    scores = jnp.where(key_live, scores, -1e+30)
    weights = jax.nn.softmax(scores, axis=-1).astype(jnp.bfloat16)
    attended = jnp.einsum('thqk,tkhd->tqhd', weights.astype(jnp.float32), value_part).astype(jnp.bfloat16)
    attended = attended.reshape(P_DEV, D_VIT)
    block_out = (group_rows.astype(jnp.float32) + jnp.dot(attended, out_weight, preferred_element_type=jnp.float32)).astype(jnp.bfloat16)
    merge_in = layer_norm(block_out, merge_gain).astype(jnp.bfloat16).reshape(M_DEV, MERGE_IN)
    hidden = jax.nn.gelu(jnp.dot(merge_in, fc1_weight, preferred_element_type=jnp.float32) + fc1_bias.astype(jnp.float32), approximate=False).astype(jnp.bfloat16)
    return (jnp.dot(hidden, fc2_weight, preferred_element_type=jnp.float32) + fc2_bias.astype(jnp.float32)).astype(jnp.bfloat16)

def reference(patches, patch_counts, dest_rows, qkv_weight, out_weight, attn_gain, merge_gain, fc1_weight, fc1_bias, fc2_weight, fc2_bias, text_embeds, section_hidden, llm_gain):
    group_total = N_SECTION * N_DP
    grouped = patches.reshape(group_total, P_DEV, D_VIT)
    grouped_counts = patch_counts.reshape(group_total, TILES_DEV)

    def one_group(pair):
        return group_embed(pair[0], pair[1], qkv_weight, out_weight, attn_gain, merge_gain, fc1_weight, fc1_bias, fc2_weight, fc2_bias)
    image_embeds = lax.map(one_group, (grouped, grouped_counts)).reshape(group_total * M_DEV, HID)
    slot_in_tile = jnp.arange(group_total * M_DEV, dtype=jnp.int32) % (BLOCK // 4)
    tile_counts = jnp.repeat(patch_counts, BLOCK // 4, total_repeat_length=group_total * M_DEV)
    live = slot_in_tile * 4 < tile_counts
    target_rows = jnp.where(live, dest_rows, group_total * SEQ_ROWS).astype(jnp.int32)
    sequence_embeds = text_embeds.at[target_rows].set(image_embeds, mode='drop')
    sectioned_seq = sequence_embeds.reshape(N_SECTION, N_DP * SEQ_ROWS, HID)
    sectioned_hidden = section_hidden.reshape(N_SECTION, N_DP * SEQ_ROWS, HID)
    entering = jnp.concatenate([sectioned_seq[:1], sectioned_hidden[:-1]], axis=0).reshape(group_total * SEQ_ROWS, HID)
    entering = entering.astype(jnp.float32)
    mean_square = lax.optimization_barrier(jnp.mean(entering * entering, axis=1, keepdims=True))
    layer_inputs = (entering * lax.rsqrt(mean_square + llm_eps) * llm_gain.astype(jnp.float32)).astype(jnp.bfloat16)
    return (sequence_embeds, layer_inputs)
```

```python
import jax
import jax.numpy as jnp
from jax import lax
from jax.sharding import PartitionSpec as P

HEAD_DIM = 80
HID = 8192
PATCHES_PER_ROW = 4
GROUP_AXES = ("section", "dp")

vit_eps = 1e-06
llm_eps = 1e-06


def from_behind(value, axis, steps):
    count = lax.axis_size(axis)
    first, last = (max(0, -steps), min(count, count - steps))
    return lax.ppermute(value, axis, [(source, source + steps) for source in range(first, last)])


def swap(value, axes, offset):
    count = lax.axis_size(axes)
    return lax.ppermute(value, axes, [(i, i ^ offset) for i in range(count)])


def layer_norm(values, gain):
    centred = values.astype(jnp.float32)
    centred = centred - jnp.mean(centred, axis=-1, keepdims=True)
    variance = jnp.mean(centred * centred, axis=-1, keepdims=True)
    return centred * lax.rsqrt(variance + vit_eps) * gain.astype(jnp.float32)


def gather_runs(block, bits, order):
    n = len(bits)
    for at in order:
        received = jnp.flip(swap(block, GROUP_AXES, bits[at]), n - 1 - at)
        block = jnp.concatenate([block, received], axis=n)
    return block


def scatter_runs(part, bits, order):
    n = len(bits)
    left = list(range(n))
    for at in order:
        axis = left.index(at)
        axis = len(left) - 1 - axis
        keep = lax.index_in_dim(part, 0, axis, keepdims=False)
        send = lax.index_in_dim(part, 1, axis, keepdims=False)
        received = swap(send.astype(jnp.bfloat16), GROUP_AXES, bits[at]).astype(jnp.float32)
        left.remove(at)
        received = jnp.flip(received, len(left) + 1 + (n - 1 - at))
        part = keep + received
    return part


def per_device(
    patches,
    patch_counts,
    dest_rows,
    qkv_weight,
    out_weight,
    attn_gain,
    merge_gain,
    fc1_weight,
    fc1_bias,
    fc2_weight,
    fc2_bias,
    text_embeds,
    section_hidden,
    llm_gain,
):
    width = patches.shape[1]
    tile_total = patch_counts.shape[0]
    block_rows = patches.shape[0] // tile_total
    merged_rows = patches.shape[0] // PATCHES_PER_ROW
    local_cols = qkv_weight.shape[2]
    local_heads = local_cols // HEAD_DIM
    feature_cols = text_embeds.shape[1]
    seq_rows = text_embeds.shape[0]
    group_count = lax.axis_size(GROUP_AXES)
    planes = lax.axis_size("mp")
    run_len = merged_rows // group_count
    group = lax.axis_index(GROUP_AXES)
    plane = lax.axis_index("mp")
    all_bits = [1 << i for i in range(group_count.bit_length() - 1)]
    pair_bit, bits = all_bits[0], all_bits[1:]
    n = len(bits)
    forward, backward = list(range(n)), list(range(n))[::-1]
    two = (2,) * n

    fc1_pair = jnp.concatenate([fc1_weight, swap(fc1_weight, GROUP_AXES, pair_bit)], axis=1)
    fc2_pair = jnp.concatenate([fc2_weight, swap(fc2_weight, GROUP_AXES, pair_bit)], axis=0)
    bias_pair = jnp.concatenate([fc1_bias, swap(fc1_bias, GROUP_AXES, pair_bit)], axis=0)

    share_bits = all_bits[:3]
    shares = 1 << len(share_bits)
    share = group % shares
    share_rows = local_cols // shares
    own_share = lax.dynamic_slice_in_dim(out_weight, share * share_rows, share_rows, 0)
    far = jnp.stack([swap(own_share, "mp", k) for k in range(1, planes)])
    halves = []
    for part, order in ((far[:, :, : width // 2], (1, 2, 0)), (far[:, :, width // 2 :], (2, 1, 0))):
        got = part[:, None, None, None]
        for at in order:
            bit = (share >> at) & 1
            received = swap(got, GROUP_AXES, share_bits[at])
            got = jnp.concatenate(
                [jnp.where(bit == 1, received, got), jnp.where(bit == 1, got, received)], axis=3 - at
            )
        halves.append(got.reshape((planes - 1) * local_cols, width // 2))
    out_full = jnp.concatenate([out_weight, jnp.concatenate(halves, axis=1)], axis=0)

    slot_in_tile = jnp.arange(merged_rows, dtype=jnp.int32) % (block_rows // PATCHES_PER_ROW)
    tile_counts = jnp.repeat(
        patch_counts, block_rows // PATCHES_PER_ROW, total_repeat_length=merged_rows
    )
    live = slot_in_tile * PATCHES_PER_ROW < tile_counts
    run_target = (dest_rows // seq_rows).reshape(group_count, run_len)[:, 0]
    place = jnp.where(live, dest_rows % seq_rows, seq_rows).reshape(group_count, run_len)
    offsets = jnp.arange(group_count, dtype=jnp.int32)
    is_run = (run_target[None, :] ^ group) == offsets[:, None]
    run_of = jnp.sum(jnp.where(is_run, offsets[None, :], 0), axis=1)

    def by_receiver(rows):
        rows = rows.reshape(group_count, run_len, -1)[run_of]
        return rows.reshape(two + (2, run_len, rows.shape[-1]))

    def of_receiver(rows):
        rows = by_receiver(rows)
        mine = rows[..., 0:1, :, :]
        theirs = swap(rows[..., 1:2, :, :], GROUP_AXES, pair_bit)
        return gather_runs(mine, bits, forward), gather_runs(theirs, bits, backward)

    def in_one_order(first, second):
        first = first.reshape(two + two + first.shape[n + 1 :])
        second = second.reshape(two + two + second.shape[n + 1 :])
        second = jnp.transpose(
            second, tuple(range(n)) + tuple(range(2 * n - 1, n - 1, -1)) + (2 * n, 2 * n + 1)
        )
        return jnp.stack([first, second], axis=n)

    place_rows = in_one_order(*of_receiver(place.reshape(merged_rows, 1)))
    place_rows = place_rows[(0,) * n].reshape(-1)

    normed_in = layer_norm(patches, attn_gain).astype(jnp.bfloat16)
    projections = jnp.dot(
        normed_in, qkv_weight.reshape(width, 3 * local_cols), preferred_element_type=jnp.float32
    ).astype(jnp.bfloat16)
    projections = projections.reshape(tile_total, block_rows, 3, local_heads, HEAD_DIM)
    query_part = projections[:, :, 0]
    key_part = projections[:, :, 1]
    value_part = projections[:, :, 2]
    scores = jnp.einsum(
        "tqhd,tkhd->thqk", query_part, key_part, preferred_element_type=jnp.float32
    ) * HEAD_DIM ** (-0.5)
    key_live = (
        jnp.arange(block_rows, dtype=jnp.int32)[None, None, None, :]
        < patch_counts[:, None, None, None]
    )
    scores = jnp.where(key_live, scores, -1e30)
    weights = jax.nn.softmax(scores, axis=-1).astype(jnp.bfloat16)
    attended = jnp.einsum(
        "thqk,tkhd->tqhd", weights, value_part, preferred_element_type=jnp.float32
    ).astype(jnp.bfloat16)
    attended = attended.reshape(merged_rows, PATCHES_PER_ROW, local_cols)

    def patch_of(values, index):
        return lax.dynamic_slice_in_dim(values, index, 1, 1).reshape(merged_rows, -1)

    heads = [patch_of(attended, plane)] + [
        swap(patch_of(attended, plane ^ k), "mp", k) for k in range(1, planes)
    ]
    proj = jnp.dot(
        jnp.concatenate(heads, axis=1), out_full, preferred_element_type=jnp.float32
    )
    own_patch = patch_of(patches.reshape(merged_rows, PATCHES_PER_ROW, width), plane)
    block_out = (own_patch.astype(jnp.float32) + proj).astype(jnp.bfloat16)
    merge_part = layer_norm(block_out, merge_gain).astype(jnp.bfloat16)

    merge_rows = in_one_order(*of_receiver(merge_part))
    merge_rows = merge_rows.reshape(-1, width)
    row_count = merge_rows.shape[0]
    first_partial = jnp.dot(merge_rows, fc1_pair, preferred_element_type=jnp.float32)
    first_partial = first_partial.reshape(planes, row_count // planes, -1)

    def chunk_of(index):
        return lax.dynamic_index_in_dim(first_partial, index, 0, keepdims=False)

    first_total = chunk_of(plane)
    for k in range(1, planes):
        first_total = first_total + swap(
            chunk_of(plane ^ k).astype(jnp.bfloat16), "mp", k
        ).astype(jnp.float32)
    hidden = jax.nn.gelu(first_total + bias_pair.astype(jnp.float32), approximate=False).astype(
        jnp.bfloat16
    )
    hidden_full = lax.all_to_all(
        jnp.broadcast_to(hidden[None], (planes,) + hidden.shape), "mp", 0, 0, tiled=True
    ).reshape(row_count, -1)

    section_hidden, _ = lax.optimization_barrier((section_hidden, merge_rows))
    incoming = from_behind(section_hidden, "section", 1)

    sides = []
    half = feature_cols // 2
    for at, order in enumerate((forward, backward)):
        side = jnp.dot(
            hidden_full,
            fc2_pair[:, at * half : (at + 1) * half],
            preferred_element_type=jnp.float32,
        )
        side = side.reshape(two + (2,) + two + (run_len, half))
        side = scatter_runs(side, bits, order).reshape(-1, half)
        side_bias = fc2_bias[at * half : (at + 1) * half].astype(jnp.float32)
        sides.append((side + side_bias).astype(jnp.bfloat16))
    embeds = jnp.concatenate(sides, axis=-1)

    hit = place_rows[None, :] == jnp.arange(seq_rows, dtype=jnp.int32)[:, None]
    placed = jnp.dot(hit.astype(jnp.bfloat16), embeds, preferred_element_type=jnp.float32)
    sequence_embeds = jnp.where(
        jnp.any(hit, axis=1, keepdims=True), placed.astype(jnp.bfloat16), text_embeds
    )
    entering = jnp.where(lax.axis_index("section") == 0, sequence_embeds, incoming).astype(
        jnp.float32
    )
    own_total = jnp.sum(entering * entering, axis=1)
    row_total = own_total
    for k in range(1, planes):
        row_total = row_total + swap(own_total, "mp", k)
    layer_inputs = (
        entering * lax.rsqrt(row_total / HID + llm_eps)[:, None] * llm_gain.astype(jnp.float32)
    ).astype(jnp.bfloat16)
    return (sequence_embeds, layer_inputs)


def solution(mesh):
    in_specs = (
        P(("section", "dp"), None),
        P(("section", "dp")),
        P(("section", "dp")),
        P(None, None, "mp"),
        P("mp", None),
        P(),
        P(),
        P("mp", ("section", "dp")),
        P(("section", "dp")),
        P(("section", "dp"), "mp"),
        P("mp"),
        P(("section", "dp"), "mp"),
        P(("section", "dp"), "mp"),
        P("mp"),
    )
    out_specs = (P(("section", "dp"), "mp"), P(("section", "dp"), "mp"))
    return jax.shard_map(
        per_device, mesh=mesh, in_specs=in_specs, out_specs=out_specs, check_vma=False
    )
```
